32 devices in a mesh: cand: 4 (over x, core), tp: 8 (over z, y).
Axes of the slice: x: 2, y: 2, z: 4, core: 2. Of those that a mesh axis runs over, the one named last changes fastest.
Arguments:
- start_state: float32 [128], replicated, may hold values from -6 to 6
- goal: float32 [128], replicated, may hold values from -6 to 6
- mean_prev: float32 [128], replicated, may hold values from -0.5 to 0.5
- std_prev: float32 [128], replicated, may hold values from 0.1 to 0.5
- noise: float32 [768, 128], P('cand'), may hold values from -23 to 23
- members: int32 [768, 1], P('cand'), may hold values from 0 to 3; in each aligned block of 192 rows (0 to 191, 192 to 383, ...) at most 60 rows name the same one
- elites: int32 [96], replicated, may hold values from 0 to 767, as said below
- w_in: bfloat16 [4, 144, 4096], P(None, None, 'tp'), may hold values from -0.5 to 0.5
- w_hid: bfloat16 [4, 4096, 4096], P(None, None, 'tp'), may hold values from -0.09375 to 0.09375
- w_out: bfloat16 [4, 4096, 128], P(None, 'tp'), may hold values from -0.09375 to 0.09375
Outputs:
- scores: float32 [768], P('cand')
- new_mean: float32 [128], replicated
- new_std: float32 [128], replicated
The draws below stay inside these ranges and needn't reach their ends.
Inputs may be any that keep to these rules, and one draw needn't show every extreme that they name: `members`: among the candidates of one index of cand no member is named more than 60 times. `elites`: 96 distinct candidate numbers.
All inputs are finite; a program needn't handle non-finite values.
Results may differ from the reference program's by a relative error of at most 0.0085.
Values may be sent and summed in bfloat16 or wider, within the bound.
A program may use at most 64 MiB of HBM per device.

```python
import math
import jax
import jax.numpy as jnp
import numpy as np
from jax import lax

H = 4096
S = 128
A = 16
HORIZON = 8
MEMBERS = 4
CAND_DEV = 192
CAP = 60
CANDS = 768
ELITES = 96
N_CAND = 4


def draw_noise(key, part):
    first_key, second_key = jax.random.split(key)
    position = jnp.arange(CANDS, dtype=jnp.float32) / max(CANDS - 1, 1)
    factor = jnp.exp(jax.random.uniform(second_key, (CANDS,), jnp.float32, math.log(0.5), math.log(1.5)))
    growth = jnp.exp(position * math.log(3.0))
    sample = jnp.clip(jax.random.normal(first_key, (CANDS, HORIZON * A), jnp.float32), -5.0, 5.0)
    return (sample * (growth * factor)[:, None]).astype(jnp.float32)


def draw_elites(key, part):
    return jax.random.permutation(jax.random.fold_in(key, 7), CANDS)[:ELITES].astype(jnp.int32)


def block_levels(own_key, dims, cuts, smallest, high):
    def one(dim, blocks):
        draws = jax.random.uniform(jax.random.fold_in(jax.random.fold_in(own_key, 6), dim), (blocks,), jnp.float32, smallest / len(cuts), high / len(cuts))
        return jnp.repeat(jnp.exp(draws), dims[dim] // blocks).reshape((-1,) + (1,) * (len(dims) - dim - 1))

    loudness = one(*cuts[0])
    for cut in cuts[1:]:
        loudness = loudness * one(*cut)
    return loudness


def shared_out(own_key, own, number, rows, amount, top, most, skew):
    ranking = jax.random.permutation(own_key, amount)
    packed, common = shares(amount, rows * top, most, skew, True), shares(amount, rows * top, most, skew, False)
    places = jnp.arange(amount)

    def named(sizes, turn):
        used = int((sizes > 0).sum())
        fixed = max(1, used // 4)
        passed = fixed + (places - fixed + turn * (used - fixed)) % max(1, amount - fixed)
        return jnp.zeros((amount,), jnp.int32).at[ranking[jnp.where(places < fixed, places, passed)]].set(jnp.asarray(sizes, jnp.int32))

    sizes = jnp.where(number % 4 == 0, named(packed, number // 4), named(common, number - number // 4 - 1))
    mixed = jax.random.permutation(jax.random.fold_in(own, 3), amount)
    source_of, receiver = mixed[0:amount // 2 * 2:2], mixed[1:amount // 2 * 2:2]
    slack = jnp.minimum(sizes[source_of] - 1, most - sizes[receiver]) // 2
    slack = jnp.where((source_of == ranking[0]) | (receiver == ranking[0]) | (sizes[receiver] == 0), 0, jnp.maximum(slack, 0))
    passed = jax.random.randint(jax.random.fold_in(own, 4), (amount // 2,), 0, 1 << 20) % (slack + 1)
    sizes = sizes.at[source_of].add(-passed).at[receiver].add(passed)
    items = jnp.searchsorted(jnp.cumsum(sizes), jnp.arange(rows * top), side="right").astype(jnp.int32)
    grid = items.reshape(top, rows).T
    grid = grid[jax.random.permutation(jax.random.fold_in(own, 1), rows)]
    turn = jax.random.randint(jax.random.fold_in(own, 2), (rows, 1), 0, top)
    return jnp.take_along_axis(grid, (jnp.arange(top)[None, :] + turn) % top, axis=1)


def shares(number_of, total, limit, slope, full):
    loads = [(1 << 20) // math.isqrt(standing ** slope) + 1 for standing in range(1, number_of + 1)]
    largest = limit if full else min(limit, max(-(-total // number_of), total * loads[0] // sum(loads)))
    least = 1 if total - largest >= number_of - 1 else 0
    given, surplus = [largest] + [least] * (number_of - 1), total - largest - least * (number_of - 1)
    while surplus > 0:
        free = [i for i in range(1, number_of) if given[i] < largest] or [i for i in range(1, number_of) if given[i] < limit]
        pool, left = sum([loads[i] for i in free]), surplus
        for i in free:
            addition = min(limit - given[i], max(1, left * loads[i] // pool), surplus)
            given[i] = given[i] + addition
            surplus = surplus - addition
    return np.array(given)


def normal_values(rng, shape, width, most, shards=(), kind=jnp.bfloat16):
    factor_of = block_levels(rng, shape, shards, -0.22, 0.18) if shards else 1.0
    drawn = jax.random.normal(rng, shape, jnp.float32) * width * factor_of
    return jnp.minimum(jnp.maximum(drawn, -most), most).astype(kind)


def setup_inputs(seed: int = 0) -> dict:
    splits = jax.random.split(jax.random.key(seed), 11)
    start_state = normal_values(splits[0], (S,), 1.0, 6.0, (), jnp.float32)
    goal = normal_values(splits[1], (S,), 1.0, 6.0, (), jnp.float32)
    mean_prev = jnp.clip(jax.random.uniform(splits[2], (HORIZON * A,), jnp.float32, -0.5, 0.5), -0.5, 0.5)
    std_prev = jnp.clip(jnp.exp(jax.random.uniform(splits[3], (HORIZON * A,), jnp.float32, math.log(0.1), math.log(0.5))), 0.1, 0.5)
    noise = draw_noise(jax.random.fold_in(splits[10], 71), 0)
    members_keys = jax.random.split(jax.random.fold_in(splits[5], 1), CANDS // CAND_DEV)
    members_turns = jax.random.permutation(jax.random.fold_in(splits[5], 3), CANDS // CAND_DEV)
    members = jax.vmap(lambda own, number: shared_out(jax.random.fold_in(splits[5], 2), own, number, CAND_DEV, MEMBERS, 1, CAP, 1))(members_keys, members_turns).reshape((CANDS, 1))
    elites = draw_elites(jax.random.fold_in(splits[10], 71), 0)
    w_in = normal_values(splits[7], (MEMBERS, S + A, H), (S + A) ** -0.5, 0.5, ((2, 8),))
    w_hid = normal_values(splits[8], (MEMBERS, H, H), H ** -0.5, 0.09375, ((2, 8),))
    w_out = normal_values(splits[9], (MEMBERS, H, S), H ** -0.5, 0.09375, ((1, 8),))
    return {"start_state": start_state, "goal": goal, "mean_prev": mean_prev, "std_prev": std_prev, "noise": noise, "members": members, "elites": elites, "w_in": w_in, "w_hid": w_hid, "w_out": w_out}


def slot_matrix(member_block, member_count, capacity):
    onehot = (member_block[:, 0:1] == jnp.arange(member_count, dtype=jnp.int32)[None, :]).astype(jnp.float32)
    before = jnp.cumsum(onehot, axis=0) - onehot
    position = lax.optimization_barrier(jnp.sum(before * onehot, axis=1)).astype(jnp.int32)
    slot_number = member_block[:, 0].astype(jnp.int32) * capacity + position
    return (slot_number[None, :] == jnp.arange(member_count * capacity, dtype=jnp.int32)[:, None]).astype(jnp.float32)

def reward_of(states, goal, action):
    return -lax.optimization_barrier(jnp.mean((states - goal[None, :]) ** 2, axis=1)) - 0.1 * lax.optimization_barrier(jnp.mean(action * action, axis=1))

def reference(start_state, goal, mean_prev, std_prev, noise, members, elites, w_in, w_hid, w_out):
    actions = mean_prev[None, :] + std_prev[None, :] * noise

    def one_block(pair):
        block_actions, block_members = pair
        dispatch = slot_matrix(block_members, MEMBERS, CAP)
        slot_actions = jnp.dot(dispatch, block_actions, precision=lax.Precision.HIGHEST)
        slot_actions = slot_actions.reshape(MEMBERS, CAP, HORIZON, A)
        gathered = []
        for member in range(MEMBERS):
            states = jnp.zeros((CAP, S), jnp.float32) + start_state[None, :]
            running = jnp.zeros((CAP,), jnp.float32)
            for step_index in range(HORIZON):
                action = slot_actions[member, :, step_index, :]
                inputs = jnp.concatenate([states, action], axis=1).astype(jnp.bfloat16)
                hidden_one = jax.nn.silu(jnp.dot(inputs, w_in[member], preferred_element_type=jnp.float32)).astype(jnp.bfloat16)
                hidden_two = jax.nn.silu(jnp.dot(hidden_one, w_hid[member], preferred_element_type=jnp.float32)).astype(jnp.bfloat16)
                change = jnp.dot(hidden_two, w_out[member], preferred_element_type=jnp.float32)
                states = states + change
                running = running + reward_of(states, goal, action)
            gathered.append(running)
        slot_returns = jnp.concatenate(gathered)
        return jnp.dot(slot_returns, dispatch, precision=lax.Precision.HIGHEST)
    returns = lax.map(one_block, (actions.reshape(N_CAND, CAND_DEV, HORIZON * A), members.reshape(N_CAND, CAND_DEV, 1)))
    returns = returns.reshape(CANDS)
    return_mean = jnp.sum(returns) / CANDS
    return_var = jnp.sum((returns - return_mean) ** 2) / CANDS
    scores = (returns - return_mean) / jnp.sqrt(return_var + 1e-06)
    chosen = jnp.zeros((CANDS,), jnp.float32).at[elites].set(1.0)
    weights = chosen * (0.5 + jax.nn.sigmoid(scores))
    weight_sum = jnp.sum(weights)
    new_mean = jnp.dot(weights, actions, precision=lax.Precision.HIGHEST) / weight_sum
    new_var = jnp.dot(weights, (actions - new_mean[None, :]) ** 2, precision=lax.Precision.HIGHEST) / weight_sum
    new_std = jnp.sqrt(new_var + 1e-06)
    return (scores, new_mean, new_std)
```

```python
import functools
import jax
import jax.numpy as jnp
from jax import lax
from jax.experimental import pallas as pl
from jax.experimental.pallas import tpu as pltpu
from jax.sharding import PartitionSpec as P

HORIZON = 8
BATCH = 128
F32 = jnp.float32
BF16 = jnp.bfloat16
HI = lax.Precision.HIGHEST


def silu_of_half(h):
    return h + h * jnp.tanh(h)


def kernel(
    n_cand, n_tp, cap,
    start_ref, goal_ref, mean_ref, std_ref, noise_ref, members_ref, elites_ref,
    win_hbm, whid_hbm, wout_hbm,
    out_ref,
    win_v, bias_v, whid_v, wout_v, h1_v, pf, rs_rx, xs, xs_send, state, sq, big,
    act_send, act_rx, sa_all, meta_all, ret_all,
    win_sem, whid_sem, wout_sem, wa_s, wa_r, bias_s, bias_r, ws_s, ws_r,
    act_s, act_r, sa_s, sa_r, meta_s, meta_r,
    rs_s, rs_r, ag_s, ag_r, ret_s, ret_r,
):
    n_mem = win_hbm.shape[0]
    depth = win_hbm.shape[1]
    chunk = win_hbm.shape[2]
    width = start_ref.shape[1]
    flat = mean_ref.shape[1]
    local = noise_ref.shape[0]
    rows = n_mem * cap
    batches = rows // BATCH
    n_work = 2 * batches
    per_batch = BATCH // cap
    lowest = n_tp // 4
    owners = range(lowest, n_tp - lowest)
    n_own = len(owners)
    own = BATCH // n_own
    a_dim = flat // HORIZON
    c = lax.axis_index("cand")
    t = lax.axis_index("tp")
    m = lax.rem(c, n_mem)
    group = c - m
    side = lax.rem(c, 2)
    first = m - side
    worker = side == 1
    owner = jnp.logical_and(t >= owners[0], t <= owners[-1])
    place_own = t - lowest
    first_own = pl.multiple_of(place_own * own, own)
    upper = t >= n_tp // 2

    def tp_peer(d):
        return lax.rem(t + d, n_tp)

    def tp_from(d):
        return lax.rem(t + n_tp - d, n_tp)

    def outer_first(i, n):
        return jnp.where(upper, i, n - 1 - i)

    def remote(src, dst, s, r, cc, tt):
        return pltpu.make_async_remote_copy(
            src_ref=src, dst_ref=dst, send_sem=s, recv_sem=r,
            device_id={"cand": cc, "tp": tt}, device_id_type=pl.DeviceIdType.MESH,
        )

    def wa_copy(mi, src, d, tt):
        return remote(
            win_hbm.at[first + mi, pl.ds(width, a_dim), :], win_v.at[mi, src, pl.ds(width, a_dim), :],
            wa_s.at[mi, d], wa_r.at[mi, src], c, tt)

    def bias_copy(mi, src, d, tt):
        return remote(bias_v.at[mi, src], bias_v.at[mi, src], bias_s.at[mi, d], bias_r.at[mi, src], c, tt)

    n_z = 4
    n_y = n_tp // n_z
    z, y = t // n_y, lax.rem(t, n_y)
    rows_s = pl.ds(0, width)

    def ws_copy(mi, src_z, e, own_slice, cc, tt):
        src = src_z * n_y + y
        held = win_hbm.at[first + mi, rows_s, :] if own_slice else win_v.at[mi, src, rows_s, :]
        return remote(held, win_v.at[mi, src, rows_s, :], ws_s.at[mi, src_z, e], ws_r.at[mi, src], cc, tt)

    def ws_own(mi, act):
        pl.when(z < n_z - 1)(act(ws_copy(mi, z, n_y, True, c, t + n_y)))
        pl.when(z > 0)(act(ws_copy(mi, z, n_y + 1, True, c, t - n_y)))
        for e in range(n_y):
            pl.when(y != e)(act(ws_copy(mi, z, e, True, c + 1, z * n_y + e)))

    def ws_relayed(mi, hop, up, act):
        src_z = z - hop if up else z + hop
        there = src_z >= 0 if up else src_z < n_z
        onward = z < n_z - 1 if up else z > 0
        beyond = ws_copy(mi, src_z, n_y if up else n_y + 1, False, c, t + n_y if up else t - n_y)
        pl.when(jnp.logical_and(there, onward))(act(beyond))
        for e in range(n_y):
            pl.when(there)(act(ws_copy(mi, src_z, e, False, c + 1, z * n_y + e)))

    def ws_arrived(mi, src):
        return remote(
            win_hbm.at[first + mi, rows_s, :], win_v.at[mi, src, rows_s, :], ws_s.at[mi, 0, 0], ws_r.at[mi, src], c, t)

    def ws_serve():
        for mi in range(2):
            ws_own(mi, lambda cp: cp.start)
        for hop in range(1, n_z):
            for mi in range(2):
                for up in (True, False):
                    src_z = z - hop if up else z + hop
                    there = src_z >= 0 if up else src_z < n_z
                    pl.when(there)(ws_arrived(mi, src_z * n_y + y).wait_recv)
                    ws_relayed(mi, hop, up, lambda cp: cp.start)

    def ws_served():
        for mi in range(2):
            ws_own(mi, lambda cp: cp.wait_send)
            for hop in range(1, n_z):
                for up in (True, False):
                    ws_relayed(mi, hop, up, lambda cp: cp.wait_send)

    def win_load(mi):
        return pltpu.make_async_copy(
            win_hbm.at[first + mi], win_v.at[mi, t, pl.ds(0, depth), :], win_sem.at[mi])

    def whid_load(mi):
        return pltpu.make_async_copy(whid_hbm.at[first + mi], whid_v.at[mi], whid_sem.at[mi])

    def wout_load(mi):
        return pltpu.make_async_copy(wout_hbm.at[first + mi], wout_v.at[mi], wout_sem.at[mi])

    @pl.when(worker)
    def _():
        for mi in range(2):
            win_load(mi).start()
        for mi in range(2):
            for d in range(1, n_tp):
                wa_copy(mi, t, d, tp_peer(d)).start()
        for mi in range(2):
            whid_load(mi).start()
            wout_load(mi).start()

    actions = mean_ref[...] + std_ref[...] * noise_ref[...]
    members = members_ref[...]
    onehot = (members == lax.broadcasted_iota(jnp.int32, (16, local), 0)).astype(F32)
    lower = (
        lax.broadcasted_iota(jnp.int32, (local, local), 0)
        < lax.broadcasted_iota(jnp.int32, (local, local), 1)
    ).astype(BF16)
    before = jnp.dot(onehot.astype(BF16), lower, preferred_element_type=F32)
    position = jnp.sum(before * onehot, axis=0, keepdims=True).astype(jnp.int32)
    slot = members * cap + position
    place_f = (slot == lax.broadcasted_iota(jnp.int32, (rows, local), 0)).astype(F32)
    act_send[...] = jnp.dot(
        place_f.astype(BF16), actions.astype(BF16), preferred_element_type=F32).astype(BF16)

    def act_copy(i):
        return remote(
            act_send.at[pl.ds(2 * i * cap, 2 * cap), :], act_rx.at[m], act_s.at[i], act_r.at[m],
            group + 2 * i + 1, t)

    for i in range(n_mem // 2):
        pl.when(c != group + 2 * i + 1)(act_copy(i).start)

    @pl.when(worker)
    def _():
        act_rx[m] = act_send[pl.ds(pl.multiple_of(first * cap, cap), 2 * cap), :]
        half_start = (0.5 * jnp.broadcast_to(start_ref[...], (16, width))).astype(BF16)
        for mi in range(2):
            win_load(mi).wait()
            bias_v[mi, t] = jnp.dot(
                half_start, win_v[mi, t, 0:width, :], preferred_element_type=F32)[0:1]
            for d in range(1, n_tp):
                bias_copy(mi, t, d, tp_peer(d)).start()

    lane = lax.broadcasted_iota(jnp.int32, (local, 128), 1)
    numbers = c * local + lax.broadcasted_iota(jnp.int32, (local, 1), 0)
    chosen = jnp.sum((numbers == elites_ref[...]).astype(F32), axis=1, keepdims=True)
    action_cost = jnp.sum(actions * actions, axis=1, keepdims=True) * (0.1 / a_dim)
    facts = jnp.where(lane == 0, 1.0, jnp.where(lane == 1, chosen, jnp.where(lane == 2, action_cost, 0.0)))
    sa_all[c] = jnp.dot(place_f, actions, precision=HI, preferred_element_type=F32)
    meta_all[c] = lax.dot_general(facts, place_f, (((0,), (1,)), ((), ())), precision=HI, preferred_element_type=F32)[:8]
    side_copies = []
    for k in range(1, n_cand):
        c2 = lax.rem(c + k, n_cand)
        side_copies.append(remote(meta_all.at[c], meta_all.at[c], meta_s.at[k], meta_r.at[k], c2, t))
        side_copies.append(remote(sa_all.at[c], sa_all.at[c], sa_s.at[k], sa_r.at[k], c2, t))
    for cp in side_copies:
        cp.start()

    pl.when(jnp.logical_not(worker))(ws_serve)

    half = min(256, chunk)

    def rs_copy(k, i, src):
        return remote(
            pf.at[k, pl.ds(pl.multiple_of(i * own, own), own), :], rs_rx.at[k, src], rs_s.at[k, i], rs_r.at[k, src],
            c, lowest + i)

    def ag_copy(k, i, dst):
        return remote(
            xs_send.at[k], xs.at[k, pl.ds(pl.multiple_of(i * own, own), own), :], ag_s.at[k, dst], ag_r.at[k, i],
            c, dst)

    lanes = lax.broadcasted_iota(jnp.int32, (1, flat), 1)

    def masked_actions(step, mi, q):
        lo = step * a_dim
        keep = jnp.where(jnp.logical_and(lanes >= lo, lanes < lo + a_dim), 0.5, 0.0).astype(BF16)
        rows_of = pl.ds(pl.multiple_of(mi * cap, cap), cap)
        acts = jnp.concatenate([act_rx[q * per_batch + b, rows_of, :] for b in range(per_batch)], axis=0)
        return acts * keep

    def contribute(k, mi):
        total = None
        for n in range(chunk // half):
            h2 = silu_of_half(0.5 * jnp.dot(
                h1_v[...], whid_v[mi, :, n * half:(n + 1) * half], preferred_element_type=F32)).astype(BF16)
            part = jnp.dot(h2, wout_v[mi, n * half:(n + 1) * half, :], preferred_element_type=F32)
            total = part if total is None else total + part
        pf[k] = total
        for i in range(n_own):
            o = outer_first(i, n_own)
            pl.when(t != lowest + o)(rs_copy(k, o, t).start)

    def reduce(k):
        change = pf[k, pl.ds(first_own, own), :]
        for d in range(1, n_tp):
            src = tp_from(d)
            rs_copy(k, 0, src).wait_recv()
            change = change + rs_rx[k, src]
        new_state = state[k] + change
        state[k] = new_state
        gap = new_state - goal_ref[...]
        sq[k] += gap * gap
        return new_state

    def broadcast(k, new_state):
        half_state = (0.5 * new_state).astype(BF16)
        xs_send[k] = half_state
        for i in range(n_tp):
            dst = outer_first(i, n_tp)
            pl.when(t != dst)(ag_copy(k, place_own, dst).start)
        xs[k, pl.ds(first_own, own), :] = half_state

    def sent_rs(k):
        for i in range(n_own):
            pl.when(t != owners[i])(rs_copy(k, i, t).wait_send)

    def sent_ag(k):
        for dst in range(n_tp):
            pl.when(t != dst)(ag_copy(k, place_own, dst).wait_send)

    @pl.when(worker)
    def _():
        state[...] = jnp.broadcast_to(start_ref[...].reshape(1, 1, width), state.shape)
        sq[...] = jnp.zeros_like(sq)
        for j in range(n_mem):
            pl.when(m != j)(remote(
                act_send.at[pl.ds(0, 2 * cap), :], act_rx.at[j], act_s.at[0], act_r.at[j], c, t).wait_recv)

        def start_work(k, mi, q):
            @pl.when(q == 0)
            def _():
                for d in range(1, n_tp):
                    src = tp_from(d)
                    wa_copy(mi, src, d, t).wait_recv()
                    bias_copy(mi, src, d, t).wait_recv()
                for d in range(n_tp):
                    tile = win_v[mi, d, width:width + a_dim, :]
                    for s in range(1, HORIZON):
                        win_v[mi, d, width + s * a_dim:width + (s + 1) * a_dim, :] = tile
                whid_load(mi).wait()
                wout_load(mi).wait()

            x = masked_actions(0, mi, q)
            for d in range(n_tp):
                h1_v[:, d * chunk:(d + 1) * chunk] = silu_of_half(
                    jnp.dot(x, win_v[mi, d, width:width + flat, :], preferred_element_type=F32)
                    + bias_v[mi, d]).astype(BF16)
            contribute(k, mi)

        def next_work(step, k, mi, q):
            @pl.when(jnp.logical_and(step == 1, q == 0))
            def _():
                for d in range(1, n_tp):
                    ws_arrived(mi, tp_from(d)).wait_recv()

            for i in range(n_own):
                pl.when(t != owners[i])(ag_copy(k, i, t).wait_recv)
            sent_rs(k)
            x = jnp.concatenate([xs[k], masked_actions(step, mi, q)], axis=1)
            for d in range(n_tp):
                h1_v[:, d * chunk:(d + 1) * chunk] = silu_of_half(
                    jnp.dot(x, win_v[mi, d], preferred_element_type=F32)).astype(BF16)
            contribute(k, mi)

        def owned(step, k):
            new_state = reduce(k)

            @pl.when(step < HORIZON - 1)
            def _():
                pl.when(step > 0)(lambda: sent_ag(k))
                broadcast(k, new_state)

        def step_body(step, carry):
            def work(k, carry):
                mi = k // batches
                q = lax.rem(k, batches)
                pl.when(step == 0)(lambda: start_work(k, mi, q))
                pl.when(step > 0)(lambda: next_work(step, k, mi, q))

                def turn(e, carry):
                    late = e == 0
                    at = jnp.where(late, step - 1, step)
                    pl.when(at >= 0)(lambda: owned(at, lax.rem(e + n_work - 1, n_work)))
                    return carry

                @pl.when(owner)
                def _():
                    lax.fori_loop(k * (k - 1) // 2, jnp.minimum(k * (k + 1) // 2, n_work), turn, 0)

                return carry

            lax.fori_loop(0, n_work, work, 0)
            return carry

        lax.fori_loop(0, HORIZON, step_body, 0)
        pl.when(owner)(lambda: owned(HORIZON - 1, n_work - 1))

    chip = c // 2
    me = (chip * n_own + place_own) * batches

    def ret_copy(src, kc, kt):
        held = ret_all.at[pl.ds(src, batches)]
        return remote(held, held, ret_s.at[kc * n_tp + kt], ret_r.at[src // batches],
                      lax.rem(c + kc, n_cand), tp_peer(kt))

    far = [(kc, kt) for kc in range(n_cand) for kt in range(n_tp) if kc + kt]
    sending = jnp.logical_and(worker, owner)

    @pl.when(sending)
    def _():
        big[...] = jnp.zeros_like(big)
        for k in range(n_work):
            at = pl.multiple_of((first + k // batches) * cap + lax.rem(first_own, cap), own)
            big[k % batches, pl.ds(at, own), :] = sq[k] * (1.0 / width)
        for q in range(batches):
            row = lax.dot_general(jnp.ones((8, width), F32), big[q], (((1,), (1,)), ((), ())),
                                  precision=HI, preferred_element_type=F32)
            ret_all[me + q] = row[0:1]
        for kc, kt in far:
            ret_copy(me, kc, kt).start()

    for cp in side_copies:
        cp.wait_recv()
    for k in range(n_cand // 2 * n_own):
        o = owners[k % n_own]
        pl.when(jnp.logical_or(t != o, c != k // n_own * 2 + 1))(ret_copy(k * batches, 0, 0).wait_recv)

    split = n_own // per_batch

    def returns_of(base, j, q, h):
        parts = [ret_all[((base // 2 + p) * n_own + h * split + i) * batches + q]
                 for p in range(n_mem // 2) for i in range(split)]
        return -functools.reduce(jnp.add, parts)

    returns = []
    for b in range(n_cand):
        j = b % n_mem
        returns.append(returns_of(b - j, j, j // per_batch, j % per_batch) - meta_all[b, 2:3, :])
    count = local * n_cand

    def over(vals):
        return jnp.sum(functools.reduce(jnp.add, vals), axis=1, keepdims=True)

    valid = [meta_all[b, 0:1, :] for b in range(n_cand)]
    mean = over([valid[b] * returns[b] for b in range(n_cand)]) / count
    var = over([valid[b] * (returns[b] - mean) ** 2 for b in range(n_cand)]) / count
    scale = jnp.sqrt(var + 1e-06)
    scores = [(returns[b] - mean) / scale for b in range(n_cand)]
    weights = [meta_all[b, 1:2, :] * (0.5 + 1.0 / (1.0 + jnp.exp(-scores[b]))) for b in range(n_cand)]
    weight_sum = over(weights)

    def moment(values):
        rows8 = [jnp.broadcast_to(weights[b], (8, rows)) for b in range(n_cand)]
        return functools.reduce(jnp.add, [
            jnp.dot(rows8[b], values(b), precision=HI, preferred_element_type=F32)
            for b in range(n_cand)])[0:1] / weight_sum

    new_mean = moment(lambda b: sa_all[b])
    out_ref[1:2, 0:flat] = new_mean
    out_ref[2:3, 0:flat] = jnp.sqrt(moment(lambda b: (sa_all[b] - new_mean) ** 2) + 1e-06)

    my_returns = returns_of(group, m, m // per_batch, lax.rem(m, per_batch)) - meta_all[c, 2:3, :]
    my_scores = jnp.broadcast_to((my_returns - mean) / scale, (8, rows))
    out_ref[0:1, 0:local] = jnp.dot(my_scores, place_f, precision=HI, preferred_element_type=F32)[0:1]

    for cp in side_copies:
        cp.wait_send()
    for i in range(n_mem // 2):
        pl.when(c != group + 2 * i + 1)(act_copy(i).wait_send)

    @pl.when(worker)
    def _():
        for mi in range(2):
            for d in range(1, n_tp):
                wa_copy(mi, t, d, tp_peer(d)).wait_send()
                bias_copy(mi, t, d, tp_peer(d)).wait_send()
        for k in range(n_work):
            sent_rs(k)

    pl.when(jnp.logical_not(worker))(ws_served)

    @pl.when(sending)
    def _():
        for k in range(n_work):
            sent_ag(k)
        for kc, kt in far:
            ret_copy(me, kc, kt).wait_send()


def unpack(packed_ref, scores_ref, new_mean_ref, new_std_ref):
    for row, ref in enumerate((scores_ref, new_mean_ref, new_std_ref)):
        ref[...] = packed_ref[row:row + 1, 0:ref.shape[1]]


def on_device(n_cand, n_tp, start_state, goal, mean_prev, std_prev, noise, members, elites, w_in, w_hid, w_out):
    local = noise.shape[0]
    n_mem, depth, chunk = w_in.shape
    width = start_state.shape[0]
    flat = mean_prev.shape[0]
    hidden = w_hid.shape[1]
    cap = -(-(5 * local // 16) // 16) * 16
    rows = n_mem * cap
    batches = rows // BATCH
    n_work = 2 * batches
    n_own = n_tp - 2 * (n_tp // 4)
    own = BATCH // n_own
    total = n_cand * n_tp
    returned = n_cand // 2 * n_own
    vmem = pl.BlockSpec(memory_space=pltpu.VMEM)
    hbm = pl.BlockSpec(memory_space=pl.ANY)
    dma = pltpu.SemaphoreType.DMA
    packed = pl.pallas_call(
        functools.partial(kernel, n_cand, n_tp, cap),
        out_shape=jax.ShapeDtypeStruct((8, max(local, flat)), F32),
        in_specs=[vmem] * 7 + [hbm] * 3,
        out_specs=vmem,
        scratch_shapes=[
            pltpu.VMEM((2, n_tp, width + flat, chunk), BF16),
            pltpu.VMEM((2, n_tp, 1, chunk), F32),
            pltpu.VMEM((2, hidden, chunk), BF16),
            pltpu.VMEM((2, chunk, width), BF16),
            pltpu.VMEM((BATCH, hidden), BF16),
            pltpu.VMEM((n_work, BATCH, width), F32),
            pltpu.VMEM((n_work, n_tp, own, width), F32),
            pltpu.VMEM((n_work, BATCH, width), BF16),
            pltpu.VMEM((n_work, own, width), BF16),
            pltpu.VMEM((n_work, own, width), F32),
            pltpu.VMEM((n_work, own, width), F32),
            pltpu.VMEM((batches, rows, width), F32),
            pltpu.VMEM((rows, flat), BF16),
            pltpu.VMEM((n_mem, 2 * cap, flat), BF16),
            pltpu.VMEM((n_cand, rows, flat), F32),
            pltpu.VMEM((n_cand, 8, rows), F32),
            pltpu.VMEM((returned * batches, 1, rows), F32),
            dma((2,)), dma((2,)), dma((2,)),
            dma((2, n_tp)), dma((2, n_tp)),
            dma((2, n_tp)), dma((2, n_tp)),
            dma((2, 4, n_tp // 4 + 2)), dma((2, n_tp)),
            dma((n_mem,)), dma((n_mem,)),
            dma((n_cand,)), dma((n_cand,)),
            dma((n_cand,)), dma((n_cand,)),
            dma((n_work, n_own)), dma((n_work, n_tp)),
            dma((n_work, n_tp)), dma((n_work, n_own)),
            dma((total,)), dma((returned,)),
        ],
        compiler_params=pltpu.CompilerParams(has_side_effects=True, vmem_limit_bytes=56 << 20),
    )(
        start_state.reshape(1, -1), goal.reshape(1, -1), mean_prev.reshape(1, -1),
        std_prev.reshape(1, -1), noise, members.reshape(1, -1), elites.reshape(1, -1), w_in, w_hid, w_out,
    )
    scores, new_mean, new_std = pl.pallas_call(
        unpack,
        out_shape=(
            jax.ShapeDtypeStruct((1, local), F32),
            jax.ShapeDtypeStruct((1, flat), F32),
            jax.ShapeDtypeStruct((1, flat), F32),
        ),
        in_specs=[vmem],
        out_specs=(vmem,) * 3,
    )(packed)
    return scores.reshape(-1), new_mean.reshape(-1), new_std.reshape(-1)


def solution(mesh):
    placed = (
        P(), P(), P(), P(), P("cand", None), P("cand", None), P(),
        P(None, None, "tp"), P(None, None, "tp"), P(None, "tp", None),
    )
    return jax.shard_map(
        functools.partial(on_device, mesh.shape["cand"], mesh.shape["tp"]),
        mesh=mesh, in_specs=placed, out_specs=(P("cand"), P(), P()), check_vma=False,
    )
```

```python
import functools
import jax
import jax.numpy as jnp
from jax import lax
from jax.experimental import pallas as pl
from jax.experimental.pallas import tpu as pltpu
from jax.sharding import PartitionSpec as P

HORIZON = 8
BATCH = 128
F32 = jnp.float32
BF16 = jnp.bfloat16
HI = lax.Precision.HIGHEST


def silu_of_half(h):
    return h + h * jnp.tanh(h)


def kernel(
    n_cand, n_tp, cap,
    start_ref, goal_ref, mean_ref, std_ref, noise_ref, members_ref, elites_ref,
    win_hbm, whid_hbm, wout_hbm,
    out_ref,
    win_v, bias_v, whid_v, wout_v, h1_v, pf, rs_rx, xs, xs_send, state, sq, big,
    act_send, act_rx, sa_all, meta_all, ret_all,
    win_sem, whid_sem, wout_sem, wa_s, wa_r, bias_s, bias_r, ws_s, ws_r,
    act_s, act_r, sa_s, sa_r, meta_s, meta_r,
    rs_s, rs_r, ag_s, ag_r, ret_s, ret_r,
):
    n_mem = win_hbm.shape[0]
    depth = win_hbm.shape[1]
    chunk = win_hbm.shape[2]
    width = start_ref.shape[1]
    flat = mean_ref.shape[1]
    local = noise_ref.shape[0]
    rows = n_mem * cap
    batches = rows // BATCH
    n_work = 2 * batches
    per_batch = BATCH // cap
    lowest = n_tp // 4
    owners = range(lowest, n_tp - lowest)
    n_own = len(owners)
    own = BATCH // n_own
    a_dim = flat // HORIZON
    c = lax.axis_index("cand")
    t = lax.axis_index("tp")
    m = lax.rem(c, n_mem)
    group = c - m
    side = lax.rem(c, 2)
    first = m - side
    worker = side == 1
    owner = jnp.logical_and(t >= owners[0], t <= owners[-1])
    place_own = t - lowest
    first_own = pl.multiple_of(place_own * own, own)
    upper = t >= n_tp // 2

    def tp_peer(d):
        return lax.rem(t + d, n_tp)

    def tp_from(d):
        return lax.rem(t + n_tp - d, n_tp)

    def outer_first(i, n):
        return jnp.where(upper, i, n - 1 - i)

    def remote(src, dst, s, r, cc, tt):
        return pltpu.make_async_remote_copy(
            src_ref=src, dst_ref=dst, send_sem=s, recv_sem=r,
            device_id={"cand": cc, "tp": tt}, device_id_type=pl.DeviceIdType.MESH,
        )

    def wa_copy(mi, src, d, tt):
        return remote(
            win_v.at[mi, src, pl.ds(width, a_dim), :], win_v.at[mi, src, pl.ds(width, a_dim), :],
            wa_s.at[mi, d], wa_r.at[mi, src], c, tt)

    def bias_copy(mi, src, d, tt):
        return remote(bias_v.at[mi, src], bias_v.at[mi, src], bias_s.at[mi, d], bias_r.at[mi, src], c, tt)

    n_z = 4
    n_y = n_tp // n_z
    z, y = t // n_y, lax.rem(t, n_y)
    rows_s = pl.ds(0, width)

    def ws_copy(mi, src_z, e, own_slice, cc, tt):
        src = src_z * n_y + y
        held = win_hbm.at[first + mi, rows_s, :] if own_slice else win_v.at[mi, src, rows_s, :]
        return remote(held, win_v.at[mi, src, rows_s, :], ws_s.at[mi, src_z, e], ws_r.at[mi, src], cc, tt)

    def ws_own(mi, act):
        pl.when(z < n_z - 1)(act(ws_copy(mi, z, n_y, True, c, t + n_y)))
        pl.when(z > 0)(act(ws_copy(mi, z, n_y + 1, True, c, t - n_y)))
        for e in range(n_y):
            pl.when(y != e)(act(ws_copy(mi, z, e, True, c + 1, z * n_y + e)))

    def ws_relayed(mi, hop, up, act):
        src_z = z - hop if up else z + hop
        there = src_z >= 0 if up else src_z < n_z
        onward = z < n_z - 1 if up else z > 0
        beyond = ws_copy(mi, src_z, n_y if up else n_y + 1, False, c, t + n_y if up else t - n_y)
        pl.when(jnp.logical_and(there, onward))(act(beyond))
        for e in range(n_y):
            pl.when(there)(act(ws_copy(mi, src_z, e, False, c + 1, z * n_y + e)))

    def ws_arrived(mi, src):
        return remote(
            win_hbm.at[first + mi, rows_s, :], win_v.at[mi, src, rows_s, :], ws_s.at[mi, 0, 0], ws_r.at[mi, src], c, t)

    def ws_serve():
        for hop in range(1, n_z):
            for mi in range(2):
                for up in (True, False):
                    src_z = z - hop if up else z + hop
                    there = src_z >= 0 if up else src_z < n_z
                    pl.when(there)(ws_arrived(mi, src_z * n_y + y).wait_recv)
                    ws_relayed(mi, hop, up, lambda cp: cp.start)

    def ws_served():
        for mi in range(2):
            ws_own(mi, lambda cp: cp.wait_send)
            for hop in range(1, n_z):
                for up in (True, False):
                    ws_relayed(mi, hop, up, lambda cp: cp.wait_send)

    def win_load(mi):
        return pltpu.make_async_copy(
            win_hbm.at[first + mi], win_v.at[mi, t, pl.ds(0, depth), :], win_sem.at[mi])

    def whid_load(mi):
        return pltpu.make_async_copy(whid_hbm.at[first + mi], whid_v.at[mi], whid_sem.at[mi])

    def wout_load(mi):
        return pltpu.make_async_copy(wout_hbm.at[first + mi], wout_v.at[mi], wout_sem.at[mi])

    entered = pltpu.get_barrier_semaphore()
    for kc in range(n_cand):
        for kt in range(n_tp):
            if kc + kt:
                pl.semaphore_signal(
                    entered, inc=1, device_id={"cand": lax.rem(c + kc, n_cand), "tp": tp_peer(kt)},
                    device_id_type=pl.DeviceIdType.MESH)

    @pl.when(worker)
    def _():
        for mi in range(2):
            win_load(mi).start()
        for mi in range(2):
            whid_load(mi).start()
            wout_load(mi).start()

    actions = mean_ref[...] + std_ref[...] * noise_ref[...]
    members = members_ref[...]
    onehot = (members == lax.broadcasted_iota(jnp.int32, (16, local), 0)).astype(F32)
    lower = (
        lax.broadcasted_iota(jnp.int32, (local, local), 0)
        < lax.broadcasted_iota(jnp.int32, (local, local), 1)
    ).astype(BF16)
    before = jnp.dot(onehot.astype(BF16), lower, preferred_element_type=F32)
    position = jnp.sum(before * onehot, axis=0, keepdims=True).astype(jnp.int32)
    slot = members * cap + position
    place_f = (slot == lax.broadcasted_iota(jnp.int32, (rows, local), 0)).astype(F32)
    act_send[...] = jnp.dot(
        place_f.astype(BF16), actions.astype(BF16), preferred_element_type=F32).astype(BF16)

    def act_copy(i):
        return remote(
            act_send.at[pl.ds(2 * i * cap, 2 * cap), :], act_rx.at[m], act_s.at[i], act_r.at[m],
            group + 2 * i + 1, t)

    @pl.when(worker)
    def _():
        act_rx[m] = act_send[pl.ds(pl.multiple_of(first * cap, cap), 2 * cap), :]
        half_start = (0.5 * jnp.broadcast_to(start_ref[...], (16, width))).astype(BF16)
        for mi in range(2):
            win_load(mi).wait()
            bias_v[mi, t] = jnp.dot(
                half_start, win_v[mi, t, 0:width, :], preferred_element_type=F32)[0:1]

    pl.semaphore_wait(entered, n_cand * n_tp - 1)
    for i in range(n_mem // 2):
        pl.when(c != group + 2 * i + 1)(act_copy(i).start)

    @pl.when(worker)
    def _():
        for mi in range(2):
            for d in range(1, n_tp):
                wa_copy(mi, t, d, tp_peer(d)).start()
                bias_copy(mi, t, d, tp_peer(d)).start()

    lane = lax.broadcasted_iota(jnp.int32, (local, 128), 1)

    @pl.when(jnp.logical_not(worker))
    def _():
        for mi in range(2):
            ws_own(mi, lambda cp: cp.start)

    numbers = c * local + lax.broadcasted_iota(jnp.int32, (local, 1), 0)
    chosen = jnp.sum((numbers == elites_ref[...]).astype(F32), axis=1, keepdims=True)
    action_cost = jnp.sum(actions * actions, axis=1, keepdims=True) * (0.1 / a_dim)
    facts = jnp.where(lane == 0, 1.0, jnp.where(lane == 1, chosen, jnp.where(lane == 2, action_cost, 0.0)))
    sa_all[c] = jnp.dot(place_f, actions, precision=HI, preferred_element_type=F32)
    meta_all[c] = lax.dot_general(facts, place_f, (((0,), (1,)), ((), ())), precision=HI, preferred_element_type=F32)[:8]
    side_copies = []
    for k in range(1, n_cand):
        c2 = lax.rem(c + k, n_cand)
        side_copies.append(remote(meta_all.at[c], meta_all.at[c], meta_s.at[k], meta_r.at[k], c2, t))
        side_copies.append(remote(sa_all.at[c], sa_all.at[c], sa_s.at[k], sa_r.at[k], c2, t))
    for cp in side_copies:
        cp.start()

    pl.when(jnp.logical_not(worker))(ws_serve)

    half = min(256, chunk)

    def rs_copy(k, i, src):
        return remote(
            pf.at[k, pl.ds(pl.multiple_of(i * own, own), own), :], rs_rx.at[k, src], rs_s.at[k, i], rs_r.at[k, src],
            c, lowest + i)

    def ag_copy(k, i, dst):
        return remote(
            xs_send.at[k], xs.at[k, pl.ds(pl.multiple_of(i * own, own), own), :], ag_s.at[k, dst], ag_r.at[k, i],
            c, dst)

    lanes = lax.broadcasted_iota(jnp.int32, (1, flat), 1)

    def masked_actions(step, mi, q):
        lo = step * a_dim
        keep = jnp.where(jnp.logical_and(lanes >= lo, lanes < lo + a_dim), 0.5, 0.0).astype(BF16)
        rows_of = pl.ds(pl.multiple_of(mi * cap, cap), cap)
        acts = jnp.concatenate([act_rx[q * per_batch + b, rows_of, :] for b in range(per_batch)], axis=0)
        return acts * keep

    def contribute(k, mi):
        total = None
        for n in range(chunk // half):
            h2 = silu_of_half(0.5 * jnp.dot(
                h1_v[...], whid_v[mi, :, n * half:(n + 1) * half], preferred_element_type=F32)).astype(BF16)
            part = jnp.dot(h2, wout_v[mi, n * half:(n + 1) * half, :], preferred_element_type=F32)
            total = part if total is None else total + part
        pf[k] = total
        for i in range(n_own):
            o = outer_first(i, n_own)
            pl.when(t != lowest + o)(rs_copy(k, o, t).start)

    def reduce(k):
        change = pf[k, pl.ds(first_own, own), :]
        for d in range(1, n_tp):
            src = tp_from(d)
            rs_copy(k, 0, src).wait_recv()
            change = change + rs_rx[k, src]
        new_state = state[k] + change
        state[k] = new_state
        gap = new_state - goal_ref[...]
        sq[k] += gap * gap
        return new_state

    def broadcast(k, new_state):
        half_state = (0.5 * new_state).astype(BF16)
        xs_send[k] = half_state
        for i in range(n_tp):
            dst = outer_first(i, n_tp)
            pl.when(t != dst)(ag_copy(k, place_own, dst).start)
        xs[k, pl.ds(first_own, own), :] = half_state

    def sent_rs(k):
        for i in range(n_own):
            pl.when(t != owners[i])(rs_copy(k, i, t).wait_send)

    def sent_ag(k):
        for dst in range(n_tp):
            pl.when(t != dst)(ag_copy(k, place_own, dst).wait_send)

    @pl.when(worker)
    def _():
        state[...] = jnp.broadcast_to(start_ref[...].reshape(1, 1, width), state.shape)
        sq[...] = jnp.zeros_like(sq)
        for j in range(n_mem):
            pl.when(m != j)(remote(
                act_send.at[pl.ds(0, 2 * cap), :], act_rx.at[j], act_s.at[0], act_r.at[j], c, t).wait_recv)

        def start_work(k, mi, q):
            @pl.when(q == 0)
            def _():
                for d in range(1, n_tp):
                    src = tp_from(d)
                    wa_copy(mi, src, d, t).wait_recv()
                    bias_copy(mi, src, d, t).wait_recv()
                for d in range(n_tp):
                    tile = win_v[mi, d, width:width + a_dim, :]
                    for s in range(1, HORIZON):
                        win_v[mi, d, width + s * a_dim:width + (s + 1) * a_dim, :] = tile
                whid_load(mi).wait()
                wout_load(mi).wait()

            x = masked_actions(0, mi, q)
            for d in range(n_tp):
                h1_v[:, d * chunk:(d + 1) * chunk] = silu_of_half(
                    jnp.dot(x, win_v[mi, d, width:width + flat, :], preferred_element_type=F32)
                    + bias_v[mi, d]).astype(BF16)
            contribute(k, mi)

        def next_work(step, k, mi, q):
            @pl.when(jnp.logical_and(step == 1, q == 0))
            def _():
                for d in range(1, n_tp):
                    ws_arrived(mi, tp_from(d)).wait_recv()

            for i in range(n_own):
                pl.when(t != owners[i])(ag_copy(k, i, t).wait_recv)
            sent_rs(k)
            x = jnp.concatenate([xs[k], masked_actions(step, mi, q)], axis=1)
            for d in range(n_tp):
                h1_v[:, d * chunk:(d + 1) * chunk] = silu_of_half(
                    jnp.dot(x, win_v[mi, d], preferred_element_type=F32)).astype(BF16)
            contribute(k, mi)

        def owned(step, k):
            new_state = reduce(k)

            @pl.when(step < HORIZON - 1)
            def _():
                pl.when(step > 0)(lambda: sent_ag(k))
                broadcast(k, new_state)

        def step_body(step, carry):
            def work(k, carry):
                mi = k // batches
                q = lax.rem(k, batches)
                pl.when(step == 0)(lambda: start_work(k, mi, q))
                pl.when(step > 0)(lambda: next_work(step, k, mi, q))

                def turn(e, carry):
                    late = e == 0
                    at = jnp.where(late, step - 1, step)
                    pl.when(at >= 0)(lambda: owned(at, lax.rem(e + n_work - 1, n_work)))
                    return carry

                @pl.when(owner)
                def _():
                    lax.fori_loop(k * (k - 1) // 2, jnp.minimum(k * (k + 1) // 2, n_work), turn, 0)

                return carry

            lax.fori_loop(0, n_work, work, 0)
            return carry

        lax.fori_loop(0, HORIZON, step_body, 0)
        pl.when(owner)(lambda: owned(HORIZON - 1, n_work - 1))

    chip = c // 2
    me = (chip * n_own + place_own) * batches

    def ret_copy(src, kc, kt):
        held = ret_all.at[pl.ds(src, batches)]
        return remote(held, held, ret_s.at[kc * n_tp + kt], ret_r.at[src // batches],
                      lax.rem(c + kc, n_cand), tp_peer(kt))

    far = [(kc, kt) for kc in range(n_cand) for kt in range(n_tp) if kc + kt]
    sending = jnp.logical_and(worker, owner)

    @pl.when(sending)
    def _():
        big[...] = jnp.zeros_like(big)
        for k in range(n_work):
            at = pl.multiple_of((first + k // batches) * cap + lax.rem(first_own, cap), own)
            big[k % batches, pl.ds(at, own), :] = sq[k] * (1.0 / width)
        for q in range(batches):
            row = lax.dot_general(jnp.ones((8, width), F32), big[q], (((1,), (1,)), ((), ())),
                                  precision=HI, preferred_element_type=F32)
            ret_all[me + q] = row[0:1]
        for kc, kt in far:
            ret_copy(me, kc, kt).start()

    for cp in side_copies:
        cp.wait_recv()
    for k in range(n_cand // 2 * n_own):
        o = owners[k % n_own]
        pl.when(jnp.logical_or(t != o, c != k // n_own * 2 + 1))(ret_copy(k * batches, 0, 0).wait_recv)

    split = n_own // per_batch

    def returns_of(base, j, q, h):
        parts = [ret_all[((base // 2 + p) * n_own + h * split + i) * batches + q]
                 for p in range(n_mem // 2) for i in range(split)]
        return -functools.reduce(jnp.add, parts)

    returns = []
    for b in range(n_cand):
        j = b % n_mem
        returns.append(returns_of(b - j, j, j // per_batch, j % per_batch) - meta_all[b, 2:3, :])
    count = local * n_cand

    def over(vals):
        return jnp.sum(functools.reduce(jnp.add, vals), axis=1, keepdims=True)

    valid = [meta_all[b, 0:1, :] for b in range(n_cand)]
    mean = over([valid[b] * returns[b] for b in range(n_cand)]) / count
    var = over([valid[b] * (returns[b] - mean) ** 2 for b in range(n_cand)]) / count
    scale = jnp.sqrt(var + 1e-06)
    scores = [(returns[b] - mean) / scale for b in range(n_cand)]
    weights = [meta_all[b, 1:2, :] * (0.5 + 1.0 / (1.0 + jnp.exp(-scores[b]))) for b in range(n_cand)]
    weight_sum = over(weights)

    def moment(values):
        rows8 = [jnp.broadcast_to(weights[b], (8, rows)) for b in range(n_cand)]
        return functools.reduce(jnp.add, [
            jnp.dot(rows8[b], values(b), precision=HI, preferred_element_type=F32)
            for b in range(n_cand)])[0:1] / weight_sum

    new_mean = moment(lambda b: sa_all[b])
    out_ref[1:2, 0:flat] = new_mean
    out_ref[2:3, 0:flat] = jnp.sqrt(moment(lambda b: (sa_all[b] - new_mean) ** 2) + 1e-06)

    my_returns = returns_of(group, m, m // per_batch, lax.rem(m, per_batch)) - meta_all[c, 2:3, :]
    my_scores = jnp.broadcast_to((my_returns - mean) / scale, (8, rows))
    out_ref[0:1, 0:local] = jnp.dot(my_scores, place_f, precision=HI, preferred_element_type=F32)[0:1]

    for cp in side_copies:
        cp.wait_send()
    for i in range(n_mem // 2):
        pl.when(c != group + 2 * i + 1)(act_copy(i).wait_send)

    @pl.when(worker)
    def _():
        for mi in range(2):
            for d in range(1, n_tp):
                wa_copy(mi, t, d, tp_peer(d)).wait_send()
                bias_copy(mi, t, d, tp_peer(d)).wait_send()
        for k in range(n_work):
            sent_rs(k)

    pl.when(jnp.logical_not(worker))(ws_served)

    @pl.when(sending)
    def _():
        for k in range(n_work):
            sent_ag(k)
        for kc, kt in far:
            ret_copy(me, kc, kt).wait_send()


def unpack(packed_ref, scores_ref, new_mean_ref, new_std_ref):
    for row, ref in enumerate((scores_ref, new_mean_ref, new_std_ref)):
        ref[...] = packed_ref[row:row + 1, 0:ref.shape[1]]


def on_device(n_cand, n_tp, start_state, goal, mean_prev, std_prev, noise, members, elites, w_in, w_hid, w_out):
    local = noise.shape[0]
    n_mem, depth, chunk = w_in.shape
    width = start_state.shape[0]
    flat = mean_prev.shape[0]
    hidden = w_hid.shape[1]
    cap = -(-(5 * local // 16) // 16) * 16
    rows = n_mem * cap
    batches = rows // BATCH
    n_work = 2 * batches
    n_own = n_tp - 2 * (n_tp // 4)
    own = BATCH // n_own
    total = n_cand * n_tp
    returned = n_cand // 2 * n_own
    vmem = pl.BlockSpec(memory_space=pltpu.VMEM)
    hbm = pl.BlockSpec(memory_space=pl.ANY)
    dma = pltpu.SemaphoreType.DMA
    packed = pl.pallas_call(
        functools.partial(kernel, n_cand, n_tp, cap),
        out_shape=jax.ShapeDtypeStruct((8, max(local, flat)), F32),
        in_specs=[vmem] * 7 + [hbm] * 3,
        out_specs=vmem,
        scratch_shapes=[
            pltpu.VMEM((2, n_tp, width + flat, chunk), BF16),
            pltpu.VMEM((2, n_tp, 1, chunk), F32),
            pltpu.VMEM((2, hidden, chunk), BF16),
            pltpu.VMEM((2, chunk, width), BF16),
            pltpu.VMEM((BATCH, hidden), BF16),
            pltpu.VMEM((n_work, BATCH, width), F32),
            pltpu.VMEM((n_work, n_tp, own, width), F32),
            pltpu.VMEM((n_work, BATCH, width), BF16),
            pltpu.VMEM((n_work, own, width), BF16),
            pltpu.VMEM((n_work, own, width), F32),
            pltpu.VMEM((n_work, own, width), F32),
            pltpu.VMEM((batches, rows, width), F32),
            pltpu.VMEM((rows, flat), BF16),
            pltpu.VMEM((n_mem, 2 * cap, flat), BF16),
            pltpu.VMEM((n_cand, rows, flat), F32),
            pltpu.VMEM((n_cand, 8, rows), F32),
            pltpu.VMEM((returned * batches, 1, rows), F32),
            dma((2,)), dma((2,)), dma((2,)),
            dma((2, n_tp)), dma((2, n_tp)),
            dma((2, n_tp)), dma((2, n_tp)),
            dma((2, 4, n_tp // 4 + 2)), dma((2, n_tp)),
            dma((n_mem,)), dma((n_mem,)),
            dma((n_cand,)), dma((n_cand,)),
            dma((n_cand,)), dma((n_cand,)),
            dma((n_work, n_own)), dma((n_work, n_tp)),
            dma((n_work, n_tp)), dma((n_work, n_own)),
            dma((total,)), dma((returned,)),
        ],
        compiler_params=pltpu.CompilerParams(
            collective_id=0, has_side_effects=True, vmem_limit_bytes=56 << 20),
    )(
        start_state.reshape(1, -1), goal.reshape(1, -1), mean_prev.reshape(1, -1),
        std_prev.reshape(1, -1), noise, members.reshape(1, -1), elites.reshape(1, -1), w_in, w_hid, w_out,
    )
    scores, new_mean, new_std = pl.pallas_call(
        unpack,
        out_shape=(
            jax.ShapeDtypeStruct((1, local), F32),
            jax.ShapeDtypeStruct((1, flat), F32),
            jax.ShapeDtypeStruct((1, flat), F32),
        ),
        in_specs=[vmem],
        out_specs=(vmem,) * 3,
    )(packed)
    return scores.reshape(-1), new_mean.reshape(-1), new_std.reshape(-1)


def solution(mesh):
    placed = (
        P(), P(), P(), P(), P("cand", None), P("cand", None), P(),
        P(None, None, "tp"), P(None, None, "tp"), P(None, "tp", None),
    )
    return jax.shard_map(
        functools.partial(on_device, mesh.shape["cand"], mesh.shape["tp"]),
        mesh=mesh, in_specs=placed, out_specs=(P("cand"), P(), P()), check_vma=False,
    )
```

```python
import functools
import jax
import jax.numpy as jnp
from jax import lax
from jax.experimental import pallas as pl
from jax.experimental.pallas import tpu as pltpu
from jax.sharding import PartitionSpec as P

HORIZON = 8
BATCH = 128
F32 = jnp.float32
BF16 = jnp.bfloat16
HI = lax.Precision.HIGHEST


def silu_of_half(h):
    return h + h * jnp.tanh(h)


def kernel(
    n_cand, n_tp, cap,
    start_ref, goal_ref, mean_ref, std_ref, noise_ref, members_ref, elites_ref,
    win_hbm, whid_hbm, wout_hbm,
    out_ref,
    win_v, bias_v, whid_v, wout_v, h1_v, pf, rs_rx, xs, xs_send, state, sq, big,
    act_send, act_rx, sa_all, meta_all, ret_all,
    win_sem, whid_sem, wout_sem, wa_s, wa_r, bias_s, bias_r, ws_s, ws_r,
    act_s, act_r, sa_s, sa_r, meta_s, meta_r,
    rs_s, rs_r, ag_s, ag_r, ret_s, ret_r,
):
    n_mem = win_hbm.shape[0]
    depth = win_hbm.shape[1]
    chunk = win_hbm.shape[2]
    width = start_ref.shape[1]
    flat = mean_ref.shape[1]
    local = noise_ref.shape[0]
    rows = n_mem * cap
    batches = rows // BATCH
    n_work = 2 * batches
    per_batch = BATCH // cap
    lowest = n_tp // 4
    owners = range(lowest, n_tp - lowest)
    n_own = len(owners)
    own = BATCH // n_own
    a_dim = flat // HORIZON
    c = lax.axis_index("cand")
    t = lax.axis_index("tp")
    m = lax.rem(c, n_mem)
    group = c - m
    side = lax.rem(c, 2)
    first = m - side
    worker = side == 1
    owner = jnp.logical_and(t >= owners[0], t <= owners[-1])
    place_own = t - lowest
    first_own = pl.multiple_of(place_own * own, own)
    upper = t >= n_tp // 2

    def tp_peer(d):
        return lax.rem(t + d, n_tp)

    def tp_from(d):
        return lax.rem(t + n_tp - d, n_tp)

    def outer_first(i, n):
        return jnp.where(upper, i, n - 1 - i)

    def remote(src, dst, s, r, cc, tt):
        return pltpu.make_async_remote_copy(
            src_ref=src, dst_ref=dst, send_sem=s, recv_sem=r,
            device_id={"cand": cc, "tp": tt}, device_id_type=pl.DeviceIdType.MESH,
        )

    def wa_copy(mi, src, d, tt):
        return remote(
            win_v.at[mi, src, pl.ds(width, a_dim), :], win_v.at[mi, src, pl.ds(width, a_dim), :],
            wa_s.at[mi, d], wa_r.at[mi, src], c, tt)

    def bias_copy(mi, src, d, tt):
        return remote(bias_v.at[mi, src], bias_v.at[mi, src], bias_s.at[mi, d], bias_r.at[mi, src], c, tt)

    n_z = 4
    n_y = n_tp // n_z
    z, y = t // n_y, lax.rem(t, n_y)
    pieces = 2
    piece = width // pieces

    def rows_s(u):
        return pl.ds(pl.multiple_of(lax.rem(u, pieces) * piece, piece), piece)

    def ws_copy(u, src_z, e, own_slice, cc, tt):
        src = src_z * n_y + y
        held = win_hbm.at[first + u // pieces, rows_s(u), :] if own_slice else win_v.at[u // pieces, src, rows_s(u), :]
        return remote(held, win_v.at[u // pieces, src, rows_s(u), :], ws_s.at[u, src_z, e], ws_r.at[u, src], cc, tt)

    def ws_own(u, act):
        pl.when(z < n_z - 1)(act(ws_copy(u, z, n_y, True, c, t + n_y)))
        pl.when(z > 0)(act(ws_copy(u, z, n_y + 1, True, c, t - n_y)))
        for e in range(n_y):
            pl.when(y != e)(act(ws_copy(u, z, e, True, c + 1, z * n_y + e)))

    def ws_relayed(u, hop, up, act):
        src_z = z - hop if up else z + hop
        there = src_z >= 0 if up else src_z < n_z
        onward = z < n_z - 1 if up else z > 0
        beyond = ws_copy(u, src_z, n_y if up else n_y + 1, False, c, t + n_y if up else t - n_y)
        pl.when(jnp.logical_and(there, onward))(act(beyond))
        for e in range(n_y):
            pl.when(there)(act(ws_copy(u, src_z, e, False, c + 1, z * n_y + e)))

    def ws_arrived(u, src):
        return remote(
            win_hbm.at[first + u // pieces, rows_s(u), :], win_v.at[u // pieces, src, rows_s(u), :], ws_s.at[u, 0, 0], ws_r.at[u, src], c, t)

    def ws_serve():
        for hop in range(1, n_z):
            for u in range(2 * pieces):
                for up in (True, False):
                    src_z = z - hop if up else z + hop
                    there = src_z >= 0 if up else src_z < n_z
                    pl.when(there)(ws_arrived(u, src_z * n_y + y).wait_recv)
                    ws_relayed(u, hop, up, lambda cp: cp.start)

    def ws_served():
        for u in range(2 * pieces):
            ws_own(u, lambda cp: cp.wait_send)
            for hop in range(1, n_z):
                for up in (True, False):
                    ws_relayed(u, hop, up, lambda cp: cp.wait_send)

    def win_load(mi):
        return pltpu.make_async_copy(
            win_hbm.at[first + mi], win_v.at[mi, t, pl.ds(0, depth), :], win_sem.at[mi])

    def whid_load(mi):
        return pltpu.make_async_copy(whid_hbm.at[first + mi], whid_v.at[mi], whid_sem.at[mi])

    def wout_load(mi):
        return pltpu.make_async_copy(wout_hbm.at[first + mi], wout_v.at[mi], wout_sem.at[mi])

    entered = pltpu.get_barrier_semaphore()
    for kc in range(n_cand):
        for kt in range(n_tp):
            if kc + kt:
                pl.semaphore_signal(
                    entered, inc=1, device_id={"cand": lax.rem(c + kc, n_cand), "tp": tp_peer(kt)},
                    device_id_type=pl.DeviceIdType.MESH)

    @pl.when(worker)
    def _():
        for mi in range(2):
            win_load(mi).start()
        for mi in range(2):
            whid_load(mi).start()
            wout_load(mi).start()

    actions = mean_ref[...] + std_ref[...] * noise_ref[...]
    members = members_ref[...]
    onehot = (members == lax.broadcasted_iota(jnp.int32, (16, local), 0)).astype(F32)
    lower = (
        lax.broadcasted_iota(jnp.int32, (local, local), 0)
        < lax.broadcasted_iota(jnp.int32, (local, local), 1)
    ).astype(BF16)
    before = jnp.dot(onehot.astype(BF16), lower, preferred_element_type=F32)
    position = jnp.sum(before * onehot, axis=0, keepdims=True).astype(jnp.int32)
    slot = members * cap + position
    place_f = (slot == lax.broadcasted_iota(jnp.int32, (rows, local), 0)).astype(F32)
    act_send[...] = jnp.dot(
        place_f.astype(BF16), actions.astype(BF16), preferred_element_type=F32).astype(BF16)

    def act_copy(i):
        return remote(
            act_send.at[pl.ds(2 * i * cap, 2 * cap), :], act_rx.at[m], act_s.at[i], act_r.at[m],
            group + 2 * i + 1, t)

    @pl.when(worker)
    def _():
        act_rx[m] = act_send[pl.ds(pl.multiple_of(first * cap, cap), 2 * cap), :]
        half_start = (0.5 * jnp.broadcast_to(start_ref[...], (16, width))).astype(BF16)
        for mi in range(2):
            win_load(mi).wait()
            bias_v[mi, t] = jnp.dot(
                half_start, win_v[mi, t, 0:width, :], preferred_element_type=F32)[0:1]

    pl.semaphore_wait(entered, n_cand * n_tp - 1)
    for i in range(n_mem // 2):
        pl.when(c != group + 2 * i + 1)(act_copy(i).start)

    @pl.when(worker)
    def _():
        for mi in range(2):
            for d in range(1, n_tp):
                wa_copy(mi, t, d, tp_peer(d)).start()
                bias_copy(mi, t, d, tp_peer(d)).start()

    lane = lax.broadcasted_iota(jnp.int32, (local, 128), 1)

    @pl.when(jnp.logical_not(worker))
    def _():
        for u in range(2 * pieces):
            ws_own(u, lambda cp: cp.start)

    numbers = c * local + lax.broadcasted_iota(jnp.int32, (local, 1), 0)
    chosen = jnp.sum((numbers == elites_ref[...]).astype(F32), axis=1, keepdims=True)
    action_cost = jnp.sum(actions * actions, axis=1, keepdims=True) * (0.1 / a_dim)
    facts = jnp.where(lane == 0, 1.0, jnp.where(lane == 1, chosen, jnp.where(lane == 2, action_cost, 0.0)))
    sa_all[c] = jnp.dot(place_f, actions, precision=HI, preferred_element_type=F32)
    meta_all[c] = lax.dot_general(facts, place_f, (((0,), (1,)), ((), ())), precision=HI, preferred_element_type=F32)[:8]
    side_copies = []
    for k in range(1, n_cand):
        c2 = lax.rem(c + k, n_cand)
        side_copies.append(remote(meta_all.at[c], meta_all.at[c], meta_s.at[k], meta_r.at[k], c2, t))
        side_copies.append(remote(sa_all.at[c], sa_all.at[c], sa_s.at[k], sa_r.at[k], c2, t))
    for cp in side_copies:
        cp.start()

    pl.when(jnp.logical_not(worker))(ws_serve)

    half = min(256, chunk)

    def rs_copy(k, i, src):
        return remote(
            pf.at[k, pl.ds(pl.multiple_of(i * own, own), own), :], rs_rx.at[k, src], rs_s.at[k, i], rs_r.at[k, src],
            c, lowest + i)

    def ag_copy(k, i, dst):
        return remote(
            xs_send.at[k], xs.at[k, pl.ds(pl.multiple_of(i * own, own), own), :], ag_s.at[k, dst], ag_r.at[k, i],
            c, dst)

    lanes = lax.broadcasted_iota(jnp.int32, (1, flat), 1)

    def masked_actions(step, mi, q):
        lo = step * a_dim
        keep = jnp.where(jnp.logical_and(lanes >= lo, lanes < lo + a_dim), 0.5, 0.0).astype(BF16)
        rows_of = pl.ds(pl.multiple_of(mi * cap, cap), cap)
        acts = jnp.concatenate([act_rx[q * per_batch + b, rows_of, :] for b in range(per_batch)], axis=0)
        return acts * keep

    def contribute(k, mi):
        total = None
        for n in range(chunk // half):
            h2 = silu_of_half(0.5 * jnp.dot(
                h1_v[...], whid_v[mi, :, n * half:(n + 1) * half], preferred_element_type=F32)).astype(BF16)
            part = jnp.dot(h2, wout_v[mi, n * half:(n + 1) * half, :], preferred_element_type=F32)
            total = part if total is None else total + part
        pf[k] = total
        for i in range(n_own):
            o = outer_first(i, n_own)
            pl.when(t != lowest + o)(rs_copy(k, o, t).start)

    def reduce(k):
        change = pf[k, pl.ds(first_own, own), :]
        for d in range(1, n_tp):
            src = tp_from(d)
            rs_copy(k, 0, src).wait_recv()
            change = change + rs_rx[k, src]
        new_state = state[k] + change
        state[k] = new_state
        gap = new_state - goal_ref[...]
        sq[k] += gap * gap
        return new_state

    def broadcast(k, new_state):
        half_state = (0.5 * new_state).astype(BF16)
        xs_send[k] = half_state
        for i in range(n_tp):
            dst = outer_first(i, n_tp)
            pl.when(t != dst)(ag_copy(k, place_own, dst).start)
        xs[k, pl.ds(first_own, own), :] = half_state

    def sent_rs(k):
        for i in range(n_own):
            pl.when(t != owners[i])(rs_copy(k, i, t).wait_send)

    def sent_ag(k):
        for dst in range(n_tp):
            pl.when(t != dst)(ag_copy(k, place_own, dst).wait_send)

    @pl.when(worker)
    def _():
        state[...] = jnp.broadcast_to(start_ref[...].reshape(1, 1, width), state.shape)
        sq[...] = jnp.zeros_like(sq)
        for j in range(n_mem):
            pl.when(m != j)(remote(
                act_send.at[pl.ds(0, 2 * cap), :], act_rx.at[j], act_s.at[0], act_r.at[j], c, t).wait_recv)

        def start_work(k, mi, q):
            @pl.when(q == 0)
            def _():
                for d in range(1, n_tp):
                    src = tp_from(d)
                    wa_copy(mi, src, d, t).wait_recv()
                    bias_copy(mi, src, d, t).wait_recv()
                for d in range(n_tp):
                    tile = win_v[mi, d, width:width + a_dim, :]
                    for s in range(1, HORIZON):
                        win_v[mi, d, width + s * a_dim:width + (s + 1) * a_dim, :] = tile
                whid_load(mi).wait()
                wout_load(mi).wait()

            x = masked_actions(0, mi, q)
            for d in range(n_tp):
                h1_v[:, d * chunk:(d + 1) * chunk] = silu_of_half(
                    jnp.dot(x, win_v[mi, d, width:width + flat, :], preferred_element_type=F32)
                    + bias_v[mi, d]).astype(BF16)
            contribute(k, mi)

        def next_work(step, k, mi, q):
            @pl.when(jnp.logical_and(step == 1, q == 0))
            def _():
                for d in range(1, n_tp):
                    for h in range(pieces):
                        ws_arrived(mi * pieces + h, tp_from(d)).wait_recv()

            for i in range(n_own):
                pl.when(t != owners[i])(ag_copy(k, i, t).wait_recv)
            sent_rs(k)
            x = jnp.concatenate([xs[k], masked_actions(step, mi, q)], axis=1)
            for d in range(n_tp):
                h1_v[:, d * chunk:(d + 1) * chunk] = silu_of_half(
                    jnp.dot(x, win_v[mi, d], preferred_element_type=F32)).astype(BF16)
            contribute(k, mi)

        def owned(step, k):
            new_state = reduce(k)

            @pl.when(step < HORIZON - 1)
            def _():
                pl.when(step > 0)(lambda: sent_ag(k))
                broadcast(k, new_state)

        def step_body(step, carry):
            def work(k, carry):
                mi = k // batches
                q = lax.rem(k, batches)
                pl.when(step == 0)(lambda: start_work(k, mi, q))
                pl.when(step > 0)(lambda: next_work(step, k, mi, q))

                def turn(e, carry):
                    late = e == 0
                    at = jnp.where(late, step - 1, step)
                    pl.when(at >= 0)(lambda: owned(at, lax.rem(e + n_work - 1, n_work)))
                    return carry

                @pl.when(owner)
                def _():
                    lax.fori_loop((k + 1) // 2, 1 + k * (k - 1) // 2, turn, 0)

                return carry

            lax.fori_loop(0, n_work, work, 0)
            return carry

        lax.fori_loop(0, HORIZON, step_body, 0)
        pl.when(owner)(lambda: owned(HORIZON - 1, n_work - 1))

    chip = c // 2
    me = (chip * n_own + place_own) * batches

    def ret_copy(src, kc, kt):
        held = ret_all.at[pl.ds(src, batches)]
        return remote(held, held, ret_s.at[kc * n_tp + kt], ret_r.at[src // batches],
                      lax.rem(c + kc, n_cand), tp_peer(kt))

    far = [(kc, kt) for kc in range(n_cand) for kt in range(n_tp) if kc + kt]
    sending = jnp.logical_and(worker, owner)

    @pl.when(sending)
    def _():
        big[...] = jnp.zeros_like(big)
        for k in range(n_work):
            at = pl.multiple_of((first + k // batches) * cap + lax.rem(first_own, cap), own)
            big[k % batches, pl.ds(at, own), :] = sq[k] * (1.0 / width)
        for q in range(batches):
            row = lax.dot_general(jnp.ones((8, width), F32), big[q], (((1,), (1,)), ((), ())),
                                  precision=HI, preferred_element_type=F32)
            ret_all[me + q] = row[0:1]
        for kc, kt in far:
            ret_copy(me, kc, kt).start()

    for cp in side_copies:
        cp.wait_recv()
    for k in range(n_cand // 2 * n_own):
        o = owners[k % n_own]
        pl.when(jnp.logical_or(t != o, c != k // n_own * 2 + 1))(ret_copy(k * batches, 0, 0).wait_recv)

    split = n_own // per_batch

    def returns_of(base, j, q, h):
        parts = [ret_all[((base // 2 + p) * n_own + h * split + i) * batches + q]
                 for p in range(n_mem // 2) for i in range(split)]
        return -functools.reduce(jnp.add, parts)

    returns = []
    for b in range(n_cand):
        j = b % n_mem
        returns.append(returns_of(b - j, j, j // per_batch, j % per_batch) - meta_all[b, 2:3, :])
    count = local * n_cand

    def over(vals):
        return jnp.sum(functools.reduce(jnp.add, vals), axis=1, keepdims=True)

    valid = [meta_all[b, 0:1, :] for b in range(n_cand)]
    mean = over([valid[b] * returns[b] for b in range(n_cand)]) / count
    var = over([valid[b] * (returns[b] - mean) ** 2 for b in range(n_cand)]) / count
    scale = jnp.sqrt(var + 1e-06)
    scores = [(returns[b] - mean) / scale for b in range(n_cand)]
    weights = [meta_all[b, 1:2, :] * (0.5 + 1.0 / (1.0 + jnp.exp(-scores[b]))) for b in range(n_cand)]
    weight_sum = over(weights)

    def moment(values):
        rows8 = [jnp.broadcast_to(weights[b], (8, rows)) for b in range(n_cand)]
        return functools.reduce(jnp.add, [
            jnp.dot(rows8[b], values(b), precision=HI, preferred_element_type=F32)
            for b in range(n_cand)])[0:1] / weight_sum

    new_mean = moment(lambda b: sa_all[b])
    out_ref[1:2, 0:flat] = new_mean
    out_ref[2:3, 0:flat] = jnp.sqrt(moment(lambda b: (sa_all[b] - new_mean) ** 2) + 1e-06)

    my_returns = returns_of(group, m, m // per_batch, lax.rem(m, per_batch)) - meta_all[c, 2:3, :]
    my_scores = jnp.broadcast_to((my_returns - mean) / scale, (8, rows))
    out_ref[0:1, 0:local] = jnp.dot(my_scores, place_f, precision=HI, preferred_element_type=F32)[0:1]

    for cp in side_copies:
        cp.wait_send()
    for i in range(n_mem // 2):
        pl.when(c != group + 2 * i + 1)(act_copy(i).wait_send)

    @pl.when(worker)
    def _():
        for mi in range(2):
            for d in range(1, n_tp):
                wa_copy(mi, t, d, tp_peer(d)).wait_send()
                bias_copy(mi, t, d, tp_peer(d)).wait_send()
        for k in range(n_work):
            sent_rs(k)

    pl.when(jnp.logical_not(worker))(ws_served)

    @pl.when(sending)
    def _():
        for k in range(n_work):
            sent_ag(k)
        for kc, kt in far:
            ret_copy(me, kc, kt).wait_send()


def unpack(packed_ref, scores_ref, new_mean_ref, new_std_ref):
    for row, ref in enumerate((scores_ref, new_mean_ref, new_std_ref)):
        ref[...] = packed_ref[row:row + 1, 0:ref.shape[1]]


def on_device(n_cand, n_tp, start_state, goal, mean_prev, std_prev, noise, members, elites, w_in, w_hid, w_out):
    local = noise.shape[0]
    n_mem, depth, chunk = w_in.shape
    width = start_state.shape[0]
    flat = mean_prev.shape[0]
    hidden = w_hid.shape[1]
    cap = -(-(5 * local // 16) // 16) * 16
    rows = n_mem * cap
    batches = rows // BATCH
    n_work = 2 * batches
    n_own = n_tp - 2 * (n_tp // 4)
    own = BATCH // n_own
    total = n_cand * n_tp
    returned = n_cand // 2 * n_own
    vmem = pl.BlockSpec(memory_space=pltpu.VMEM)
    hbm = pl.BlockSpec(memory_space=pl.ANY)
    dma = pltpu.SemaphoreType.DMA
    packed = pl.pallas_call(
        functools.partial(kernel, n_cand, n_tp, cap),
        out_shape=jax.ShapeDtypeStruct((8, max(local, flat)), F32),
        in_specs=[vmem] * 7 + [hbm] * 3,
        out_specs=vmem,
        scratch_shapes=[
            pltpu.VMEM((2, n_tp, width + flat, chunk), BF16),
            pltpu.VMEM((2, n_tp, 1, chunk), F32),
            pltpu.VMEM((2, hidden, chunk), BF16),
            pltpu.VMEM((2, chunk, width), BF16),
            pltpu.VMEM((BATCH, hidden), BF16),
            pltpu.VMEM((n_work, BATCH, width), F32),
            pltpu.VMEM((n_work, n_tp, own, width), F32),
            pltpu.VMEM((n_work, BATCH, width), BF16),
            pltpu.VMEM((n_work, own, width), BF16),
            pltpu.VMEM((n_work, own, width), F32),
            pltpu.VMEM((n_work, own, width), F32),
            pltpu.VMEM((batches, rows, width), F32),
            pltpu.VMEM((rows, flat), BF16),
            pltpu.VMEM((n_mem, 2 * cap, flat), BF16),
            pltpu.VMEM((n_cand, rows, flat), F32),
            pltpu.VMEM((n_cand, 8, rows), F32),
            pltpu.VMEM((returned * batches, 1, rows), F32),
            dma((2,)), dma((2,)), dma((2,)),
            dma((2, n_tp)), dma((2, n_tp)),
            dma((2, n_tp)), dma((2, n_tp)),
            dma((4, 4, n_tp // 4 + 2)), dma((4, n_tp)),
            dma((n_mem,)), dma((n_mem,)),
            dma((n_cand,)), dma((n_cand,)),
            dma((n_cand,)), dma((n_cand,)),
            dma((n_work, n_own)), dma((n_work, n_tp)),
            dma((n_work, n_tp)), dma((n_work, n_own)),
            dma((total,)), dma((returned,)),
        ],
        compiler_params=pltpu.CompilerParams(
            collective_id=0, has_side_effects=True, vmem_limit_bytes=56 << 20),
    )(
        start_state.reshape(1, -1), goal.reshape(1, -1), mean_prev.reshape(1, -1),
        std_prev.reshape(1, -1), noise, members.reshape(1, -1), elites.reshape(1, -1), w_in, w_hid, w_out,
    )
    scores, new_mean, new_std = pl.pallas_call(
        unpack,
        out_shape=(
            jax.ShapeDtypeStruct((1, local), F32),
            jax.ShapeDtypeStruct((1, flat), F32),
            jax.ShapeDtypeStruct((1, flat), F32),
        ),
        in_specs=[vmem],
        out_specs=(vmem,) * 3,
    )(packed)
    return scores.reshape(-1), new_mean.reshape(-1), new_std.reshape(-1)


def solution(mesh):
    placed = (
        P(), P(), P(), P(), P("cand", None), P("cand", None), P(),
        P(None, None, "tp"), P(None, None, "tp"), P(None, "tp", None),
    )
    return jax.shard_map(
        functools.partial(on_device, mesh.shape["cand"], mesh.shape["tp"]),
        mesh=mesh, in_specs=placed, out_specs=(P("cand"), P(), P()), check_vma=False,
    )
```
